128 devices in a mesh: section: 8 (over x, core), tp: 16 (over z, y).
Axes of the slice: x: 4, y: 4, z: 4, core: 2. Of those that a mesh axis runs over, the one named last changes fastest.
Arguments:
- pending_activation: bfloat16 [8, 128, 4096], P('section'), may hold values from -6 to 6
- admissible_microbatches: bfloat16 [4, 128, 4096], P(None, None, 'tp'), may hold values from -6 to 6
- arrival_plan: int32 [4], replicated, may hold values from 0 to 3, each once
- vanished_hop: int32 [1], replicated, may hold values from 1 to 7
- query_key_value_matrices: bfloat16 [8, 4096, 3, 2048], P('section', None, None, 'tp')
- mixing_projection_matrices: bfloat16 [8, 2048, 4096], P('section', 'tp'), may hold values from -0.125 to 0.125
- normalizer_factors: bfloat16 [8, 4096], P('section'), may hold values from 0.25 to 1.75
Outputs:
- activation_later: bfloat16 [8, 128, 4096], P('section')
- standby_input: bfloat16 [8, 128, 4096], P('section', None, 'tp')
The draws below stay inside these ranges and needn't reach their ends.
Inputs may be any that keep to these rules, and one draw needn't show every extreme that they name: `vanished_hop`: the preempted section is not the first. `arrival_plan`: each micro-batch index once.
All inputs are finite; a program needn't handle non-finite values.
Results may differ from the reference program's by a relative error of at most 0.013.
Values may be sent and summed in bfloat16 or wider, within the bound.
A program may use at most 64 MiB of HBM per device.

```python
import jax
import jax.numpy as jnp
from jax import lax

HIDDEN_SIZE = 4096
HEADS = 16
HD = 128
STRING_LENGTH = 128
TICKS = 3
POOL = 4
LAYER_HOPS = 8


def draw_query_key_value_matrices(key, part):
    base = jax.random.normal(key, (LAYER_HOPS, HIDDEN_SIZE, 3, HEADS * HD), jnp.float32) * HIDDEN_SIZE ** (-0.5)
    return base.astype(jnp.bfloat16)


def level_of(stream_key, dims, pieces, low, high):
    loudness = 1.0
    for position, shards_of in pieces:
        draws = jax.random.uniform(jax.random.fold_in(jax.random.fold_in(stream_key, 6), position), (shards_of,), jnp.float32, low / len(pieces), high / len(pieces))
        loudness = loudness * jnp.repeat(jnp.exp(draws), dims[position] // shards_of).reshape((-1,) + (1,) * (len(dims) - 1 - position))
    return loudness


def bell_draw(rng, dims, width, limit, cuts=(), held_as=jnp.bfloat16):
    array = jax.random.normal(rng, dims, jnp.float32) * width
    if len(cuts) > 0:
        array = level_of(rng, dims, cuts, -0.22, 0.18) * array
    return jnp.clip(array, min=-limit, max=limit).astype(held_as)


def setup_inputs(seed: int = 0) -> dict:
    arg_keys = jax.random.split(jax.random.key(seed), 8)
    pending_activation = bell_draw(arg_keys[0], (LAYER_HOPS, STRING_LENGTH, HIDDEN_SIZE), 1.0, 6.0, ((0, 8),))
    admissible_microbatches = bell_draw(arg_keys[1], (POOL, STRING_LENGTH, HIDDEN_SIZE), 1.0, 6.0, ((2, 16),))
    arrival_plan = jax.random.permutation(arg_keys[2], POOL).astype(jnp.int32)
    vanished_hop = jax.random.randint(arg_keys[3], (1,), 1, LAYER_HOPS).astype(jnp.int32)
    query_key_value_matrices = draw_query_key_value_matrices(jax.random.fold_in(arg_keys[7], 71), 0)
    mixing_projection_matrices = bell_draw(arg_keys[5], (LAYER_HOPS, HEADS * HD, HIDDEN_SIZE), (HEADS * HD) ** -0.5, 0.125, ((0, 8), (1, 16)))
    normalizer_factors = jnp.clip(1.0 + 0.15 * jax.random.normal(arg_keys[6], (LAYER_HOPS, HIDDEN_SIZE), jnp.float32), 0.25, 1.75).astype(jnp.bfloat16)
    return dict(pending_activation=pending_activation, admissible_microbatches=admissible_microbatches, arrival_plan=arrival_plan, vanished_hop=vanished_hop, query_key_value_matrices=query_key_value_matrices, mixing_projection_matrices=mixing_projection_matrices, normalizer_factors=normalizer_factors)


NORM_EPS = 1e-05

def layer_norm(x_rows, scale_row):
    widened = x_rows.astype(jnp.float32)
    row_mean = lax.optimization_barrier(jnp.mean(widened, axis=-1, keepdims=True))
    centered = widened - row_mean
    row_var = lax.optimization_barrier(jnp.mean(centered * centered, axis=-1, keepdims=True))
    return (centered * lax.rsqrt(row_var + NORM_EPS) * scale_row.astype(jnp.float32)).astype(jnp.bfloat16)

def attend(normed, w_in, w_out):
    row_count = normed.shape[0]
    col_count = w_in.shape[2]
    head_count = col_count // HD
    projected = jnp.dot(normed, w_in.reshape(w_in.shape[0], 3 * col_count), preferred_element_type=jnp.float32)
    projected = projected.astype(jnp.bfloat16).reshape(row_count, 3, head_count, HD)
    queries = projected[:, 0].astype(jnp.float32)
    key_rows = projected[:, 1].astype(jnp.float32)
    values = projected[:, 2].astype(jnp.float32)
    scores = jnp.einsum('qhd,khd->hqk', queries, key_rows) * HD ** (-0.5)
    causal = jnp.arange(row_count)[:, None] >= jnp.arange(row_count)[None, :]
    scores = jnp.where(causal[None], scores, -jnp.inf)
    row_max = lax.optimization_barrier(jnp.max(scores, axis=-1, keepdims=True))
    weights = jnp.exp(scores - row_max)
    probs = (weights / lax.optimization_barrier(jnp.sum(weights, axis=-1, keepdims=True))).astype(jnp.bfloat16)
    context = jnp.einsum('hqk,khd->qhd', probs.astype(jnp.float32), values)
    context = context.astype(jnp.bfloat16).reshape(row_count, col_count)
    return jnp.dot(context, w_out, preferred_element_type=jnp.float32)

def section_layer(x_rows, w_in, w_out, scale_row):
    branch = attend(layer_norm(x_rows, scale_row), w_in, w_out)
    return (x_rows.astype(jnp.float32) + branch).astype(jnp.bfloat16)

def reference(pending_activation, admissible_microbatches, arrival_plan, vanished_hop, query_key_value_matrices, mixing_projection_matrices, normalizer_factors):
    lost_at = vanished_hop[0]
    section_ids = jnp.arange(LAYER_HOPS)[:, None, None]
    activation_later = pending_activation
    spares = None
    for tick_index in range(TICKS):
        outputs = lax.map(lambda operands: section_layer(*operands), (activation_later, query_key_value_matrices, mixing_projection_matrices, normalizer_factors))
        if tick_index == TICKS - 1:
            spares = lax.map(lambda operands: section_layer(*operands), (outputs, jnp.roll(query_key_value_matrices, -1, axis=0), jnp.roll(mixing_projection_matrices, -1, axis=0), jnp.roll(normalizer_factors, -1, axis=0)))
            redone = lax.dynamic_index_in_dim(spares, lost_at - 1, 0, keepdims=False)
        else:
            earlier = lax.dynamic_index_in_dim(outputs, lost_at - 1, 0, keepdims=False)
            redone = section_layer(earlier, lax.dynamic_index_in_dim(query_key_value_matrices, lost_at, 0, keepdims=False), lax.dynamic_index_in_dim(mixing_projection_matrices, lost_at, 0, keepdims=False), lax.dynamic_index_in_dim(normalizer_factors, lost_at, 0, keepdims=False))
        outputs = lax.dynamic_update_index_in_dim(outputs, redone, lost_at - 1, 0)
        entering = lax.dynamic_index_in_dim(admissible_microbatches, arrival_plan[tick_index], 0, keepdims=True)
        shifted = jnp.concatenate([entering, outputs[:-1]], axis=0)
        activation_later = jnp.where(section_ids == lost_at, jnp.zeros_like(shifted), jnp.where(section_ids == lost_at + 1, redone[None], shifted))
    standby_input = jnp.roll(spares, 2, axis=0)
    return (activation_later, standby_input)
```

```python
import jax
import jax.numpy as jnp
from jax import lax
from jax.sharding import PartitionSpec as P

HD = 128
NORM_EPS = 1e-05


def shifted(value, axis, steps):
    count = lax.axis_size(axis)
    pairs = [(source, (source + steps) % count) for source in range(count)]
    return lax.ppermute(value, axis, pairs)


def from_everyone(array, axis):
    copies = jnp.broadcast_to(array, (lax.axis_size(axis), *array.shape))
    return lax.all_to_all(copies, axis, split_axis=0, concat_axis=0, tiled=True)


def gather_columns(array, axis):
    blocks = from_everyone(array, axis)
    return jnp.moveaxis(blocks, 0, 1).reshape(array.shape[0], -1)


def layer_norm(x_rows, scale_row):
    widened = x_rows.astype(jnp.float32)
    row_mean = jnp.mean(widened, axis=-1, keepdims=True)
    centered = widened - row_mean
    row_var = jnp.mean(centered * centered, axis=-1, keepdims=True)
    return (centered * lax.rsqrt(row_var + NORM_EPS) * scale_row.astype(jnp.float32)).astype(
        jnp.bfloat16
    )


def context_of(normed, w_in):
    rows = normed.shape[0]
    projected = jnp.dot(
        normed, w_in.reshape(w_in.shape[0], -1), preferred_element_type=jnp.float32
    ).astype(jnp.bfloat16)
    q, k, v = (projected[:, i * HD : (i + 1) * HD] for i in range(3))
    scores = jnp.dot(q, k.T, preferred_element_type=jnp.float32) * HD ** (-0.5)
    causal = jnp.arange(rows)[:, None] >= jnp.arange(rows)[None, :]
    scores = jnp.where(causal, scores, -jnp.inf)
    weights = jnp.exp(scores - jnp.max(scores, axis=-1, keepdims=True))
    probs = (weights / jnp.sum(weights, axis=-1, keepdims=True)).astype(jnp.bfloat16)
    return jnp.dot(probs, v, preferred_element_type=jnp.float32).astype(jnp.bfloat16)


def per_device(pending, admissible, plan, vanished_hop, w_in, w_out, gain):
    last = lax.axis_size("section") - 1
    sections = last + 1
    me = lax.axis_index("section")
    tp = lax.axis_size("tp")
    width = pending.shape[2] // tp
    lost = vanished_hop[0]
    w_in, w_out, gain = w_in[0], w_out[0], gain[0]
    depth = w_out.shape[0]
    by_column = lax.all_to_all(
        jnp.moveaxis(w_out.reshape(depth, tp, width), 1, 0), "tp", 0, 0, tiled=True
    ).reshape(tp * depth, width)
    x_full = jnp.where(me == lost, 0, pending[0]).astype(jnp.bfloat16)
    x_sh = lax.dynamic_slice_in_dim(x_full, lax.axis_index("tp") * width, width, 1)
    entering = [lax.dynamic_index_in_dim(admissible, plan[i], 0, keepdims=False) for i in range(3)]
    late_wrap = (lost == last - 1) | (lost == last - 2)
    ys, fulls = [], []
    for slot in range(5):
        context = gather_columns(context_of(layer_norm(x_full, gain), w_in), "tp")
        y = x_sh.astype(jnp.float32) + jnp.dot(
            context, by_column, preferred_element_type=jnp.float32
        )
        y = y.astype(jnp.bfloat16)
        ys.append(y)
        if slot == 4:
            break
        if slot < 2:
            wrapped = entering[slot]
        elif slot == 2:
            wrapped = jnp.where(late_wrap, entering[2], jnp.where(lost == last, ys[0], y))
        else:
            wrapped = jnp.where(late_wrap, y, entering[2])
        x_sh = shifted(jnp.where(me == last, wrapped, y), "section", 1)
        x_full = gather_columns(x_sh, "tp")
        fulls.append(x_full)
    x4, x5 = fulls[2], fulls[3]
    use5 = jnp.where(me == 0, ~late_wrap, (me > lost) & (me <= lost + 3))
    out = jnp.where(me == lost, 0, jnp.where(use5, x5, x4)).astype(jnp.bfloat16)
    dest = (me + 1) % sections
    early = (dest == (lost + 2) % sections) & (lost <= last - 1)
    late = ((dest == (lost + 3) % sections) & (lost <= last - 1)) | (
        (dest == (lost + 4) % sections) & (lost <= last - 2)
    )
    spare = jnp.where(early, ys[1], jnp.where(late, ys[4], ys[3]))
    return out[None], shifted(spare, "section", 1)[None]


def solution(mesh):
    placed = (
        P("section", None, None),
        P(None, None, "tp"),
        P(),
        P(),
        P("section", None, None, "tp"),
        P("section", "tp", None),
        P("section", None),
    )
    return jax.shard_map(
        per_device,
        mesh=mesh,
        in_specs=placed,
        out_specs=(P("section", None, None), P("section", None, "tp")),
        check_vma=False,
    )
```

```python
import functools

import jax
import jax.numpy as jnp
from jax import lax
from jax.experimental import pallas as pl
from jax.experimental.pallas import tpu as pltpu
from jax.sharding import PartitionSpec as P

HD = 128
LANES = 128
SLOTS = 5
CHUNKS = 2
NORM_EPS = 1e-05
MESH = pl.DeviceIdType.MESH


def arrive(ref, sem):
    pltpu.make_async_copy(ref, ref, sem).wait()


def kernel(
    side,
    pending,
    admissible,
    plan,
    vanished,
    w_in_hbm,
    w_out_hbm,
    gain,
    out_ref,
    standby_ref,
    x_raw,
    w_in,
    w_out,
    x,
    ctx,
    y_real,
    y_send,
    normed,
    keys,
    values,
    spare,
    load_sem,
    wo_sem,
    ctx_sem,
    one_sem,
    two_sem,
    end_sem,
):
    sections = lax.axis_size("section")
    section = lax.axis_index("section")
    tp = lax.axis_index("tp")
    count = side * side
    z, y = tp // side, tp % side
    following = (section + 1) % sections
    rows, width = pending.shape[0], pending.shape[1]
    part = rows // CHUNKS
    cols = width // count
    halves = cols // LANES
    lost = vanished[0]
    final = sections - 1
    late_wrap = (lost == final - 1) | (lost == final - 2)

    def send(src, dst, sems, where):
        copy = pltpu.make_async_remote_copy(
            src_ref=src,
            dst_ref=dst,
            send_sem=sems.at[0],
            recv_sem=sems.at[1],
            device_id=where,
            device_id_type=MESH,
        )
        copy.start()

    def others(dz, dy):
        return ((z + dz) % side) * side + (y + dy) % side

    steps = [(a, b) for a in range(side) for b in range(side) if a or b]

    load_x = pltpu.make_async_copy(pending, x_raw, load_sem.at[0])
    load_x.start()
    loads = [
        pltpu.make_async_copy(
            w_in_hbm.at[j], w_in.at[:, pl.ds(j * HD, HD)], load_sem.at[1 + j]
        )
        for j in range(3)
    ]
    for load in loads:
        load.start()
    own = pltpu.make_async_copy(
        w_out_hbm.at[:, pl.ds(pl.multiple_of(tp * cols, LANES), cols)], w_out.at[tp], load_sem.at[4]
    )
    own.start()
    for dz, dy in steps:
        peer = others(dz, dy)
        send(
            w_out_hbm.at[:, pl.ds(pl.multiple_of(peer * cols, LANES), cols)],
            w_out.at[tp],
            wo_sem,
            (section, peer),
        )
    load_x.wait()
    for c in range(count):
        for h in range(halves):
            for r in range(CHUNKS):
                block = x_raw[r * part : (r + 1) * part, c * cols + h * LANES : c * cols + (h + 1) * LANES]
                x[0, r, h, c // side, c % side] = jnp.where(section == lost, jnp.zeros_like(block), block)
    for load in loads:
        load.wait()

    def heads(k, r):
        def blocks():
            for c in range(count):
                for h in range(halves):
                    yield c * cols + h * LANES, x[k, r, h, c // side, c % side].astype(jnp.float32)

        total = jnp.zeros((part, LANES), jnp.float32)
        for _, block in blocks():
            total = total + block
        mean = jnp.sum(total, axis=-1, keepdims=True) * (1.0 / width)
        total = jnp.zeros((part, LANES), jnp.float32)
        for _, block in blocks():
            block = block - mean
            total = total + block * block
        scale = lax.rsqrt(jnp.sum(total, axis=-1, keepdims=True) * (1.0 / width) + NORM_EPS)
        for at, block in blocks():
            g = gain[:, at : at + LANES].astype(jnp.float32)
            normed[:, at : at + LANES] = ((block - mean) * scale * g).astype(jnp.bfloat16)
        projected = jnp.dot(normed[...], w_in[...], preferred_element_type=jnp.float32).astype(
            jnp.bfloat16
        )
        keys[r * part : (r + 1) * part, :] = projected[:, HD : 2 * HD]
        values[r * part : (r + 1) * part, :] = projected[:, 2 * HD :]
        seen = (r + 1) * part
        scores = lax.dot_general(
            projected[:, :HD],
            keys[:seen, :],
            (((1,), (1,)), ((), ())),
            preferred_element_type=jnp.float32,
        ) * HD ** (-0.5)
        row = lax.broadcasted_iota(jnp.int32, (part, seen), 0) + r * part
        col = lax.broadcasted_iota(jnp.int32, (part, seen), 1)
        scores = jnp.where(row >= col, scores, -jnp.inf)
        weights = jnp.exp(scores - jnp.max(scores, axis=-1, keepdims=True))
        probs = (weights / jnp.sum(weights, axis=-1, keepdims=True)).astype(jnp.bfloat16)
        mixed = jnp.dot(probs, values[:seen, :], preferred_element_type=jnp.float32)
        ctx[k, r, tp] = mixed.astype(jnp.bfloat16)
        for dz, dy in steps:
            send(ctx.at[k, r, tp], ctx.at[k, r, tp], ctx_sem.at[k, r], (section, others(dz, dy)))

    def mix(k, r):
        arrive(ctx.at[k, r, pl.ds(0, count - 1)], ctx_sem.at[k, r, 1])
        context = jnp.concatenate([ctx[k, r, i] for i in range(count)], axis=1)
        weights = w_out[...].reshape(count * HD, cols)
        branch = jnp.dot(context, weights, preferred_element_type=jnp.float32)
        mine = jnp.concatenate([x[k, r, h, z, y] for h in range(halves)], axis=1)
        result = (mine.astype(jnp.float32) + branch).astype(jnp.bfloat16)
        y_real[k, r] = result

        @pl.when(k < SLOTS - 1)
        def _():
            entering = admissible[plan[jnp.minimum(k, 2)], r * part : (r + 1) * part, :]
            enters = (k < 2) | ((k == 2) & late_wrap) | ((k == 3) & jnp.logical_not(late_wrap))
            held = jnp.where((k == 2) & (lost == final), y_real[0, r], result)
            wrapped = jnp.where(enters, entering, held)
            sent = jnp.where(section == final, wrapped, result)
            for h in range(halves):
                y_send[k, r, h] = sent[:, h * LANES : (h + 1) * LANES]
                for step in range(side):
                    peer = others(step, 0) if h == 0 else others(0, step)
                    send(
                        y_send.at[k, r, h],
                        x.at[k + 1, r, h, z, y],
                        one_sem.at[k, r, h],
                        (following, peer),
                    )

    def line(k, r, h):
        return x.at[k + 1, r, h, :, y] if h == 0 else x.at[k + 1, r, h, z]

    def forward(k, r):
        for h in range(halves):
            arrive(x.at[k + 1, r, h, 0], one_sem.at[k, r, h, 1])
            for step in range(1, side):
                peer = others(0, step) if h == 0 else others(step, 0)
                send(line(k, r, h), line(k, r, h), two_sem.at[k, r, h], (section, peer))

    def gathered(k, r):
        for h in range(halves):
            arrive(x.at[k + 1, r, h, pl.ds(0, side - 1)], two_sem.at[k, r, h, 1])

    def slot(k, carry):
        for r in range(CHUNKS):

            @pl.when(k > 0)
            def _():
                gathered(k - 1, r)

            heads(k, r)

        @pl.when(k == 0)
        def _():
            own.wait()
            arrive(w_out.at[pl.ds(0, count - 1)], wo_sem.at[1])

        @pl.when(k == SLOTS - 1)
        def _():
            behind = (section > lost) & (section <= lost + 3)
            newest = jnp.where(section == 0, jnp.logical_not(late_wrap), behind)
            for c in range(count):
                for h in range(halves):
                    for r in range(CHUNKS):
                        at = (r, h, c // side, c % side)
                        block = jnp.where(newest, x[SLOTS - 1, *at], x[SLOTS - 2, *at])
                        block = jnp.where(section == lost, jnp.zeros_like(block), block)
                        start = c * cols + h * LANES
                        out_ref[r * part : (r + 1) * part, start : start + LANES] = block

        for r in range(CHUNKS):
            mix(k, r)

        @pl.when(k < SLOTS - 1)
        def _():
            for r in range(CHUNKS):
                forward(k, r)

        return carry

    lax.fori_loop(0, SLOTS, slot, 0)

    target = (section + 1) % sections
    early = (target == (lost + 2) % sections) & (lost <= final - 1)
    late = ((target == (lost + 3) % sections) & (lost <= final - 1)) | (
        (target == (lost + 4) % sections) & (lost <= final - 2)
    )
    for r in range(CHUNKS):
        chosen = jnp.where(early, y_real[1, r], jnp.where(late, y_real[4, r], y_real[3, r]))
        spare[r] = chosen
        send(spare.at[r], standby_ref.at[pl.ds(r * part, part)], end_sem.at[r], (following, tp))

    arrive(w_out.at[pl.ds(0, count - 1)], wo_sem.at[0])

    def drain(k, carry):
        for r in range(CHUNKS):
            arrive(ctx.at[k, r, pl.ds(0, count - 1)], ctx_sem.at[k, r, 0])

            @pl.when(k < SLOTS - 1)
            def _():
                for h in range(halves):
                    arrive(x.at[k, r, h, 0], one_sem.at[k, r, h, 0])
                    arrive(x.at[k, r, h, pl.ds(0, side - 1)], two_sem.at[k, r, h, 0])

        return carry

    lax.fori_loop(0, SLOTS, drain, 0)
    for r in range(CHUNKS):
        arrive(spare.at[r], end_sem.at[r, 0])
        arrive(spare.at[r], end_sem.at[r, 1])


def per_device(pending, admissible, plan, vanished_hop, w_in, w_out, gain):
    count = lax.axis_size("tp")
    side = int(round(count**0.5))
    rows, width = pending.shape[1:]
    cols = width // count
    part = rows // CHUNKS
    halves = cols // LANES
    vmem = pl.BlockSpec(memory_space=pltpu.VMEM)
    smem = pl.BlockSpec(memory_space=pltpu.SMEM)
    anywhere = pl.BlockSpec(memory_space=pl.ANY)
    bf16 = jnp.bfloat16
    dma = pltpu.SemaphoreType.DMA
    out, standby = pl.pallas_call(
        functools.partial(kernel, side),
        out_shape=(
            jax.ShapeDtypeStruct((rows, width), bf16),
            jax.ShapeDtypeStruct((rows, cols), bf16),
        ),
        in_specs=[anywhere, vmem, smem, smem, anywhere, anywhere, vmem],
        out_specs=(vmem, anywhere),
        scratch_shapes=[
            pltpu.VMEM((rows, width), bf16),
            pltpu.VMEM((width, 3 * HD), bf16),
            pltpu.VMEM((count, HD, cols), bf16),
            pltpu.VMEM((SLOTS, CHUNKS, halves, side, side, part, LANES), bf16),
            pltpu.VMEM((SLOTS, CHUNKS, count, part, HD), bf16),
            pltpu.VMEM((SLOTS, CHUNKS, part, cols), bf16),
            pltpu.VMEM((SLOTS - 1, CHUNKS, halves, part, LANES), bf16),
            pltpu.VMEM((part, width), bf16),
            pltpu.VMEM((rows, HD), bf16),
            pltpu.VMEM((rows, HD), bf16),
            pltpu.VMEM((CHUNKS, part, cols), bf16),
            dma((5,)),
            dma((2,)),
            dma((SLOTS, CHUNKS, 2)),
            dma((SLOTS - 1, CHUNKS, halves, 2)),
            dma((SLOTS - 1, CHUNKS, halves, 2)),
            dma((CHUNKS, 2)),
        ],
        compiler_params=pltpu.CompilerParams(
            has_side_effects=True, vmem_limit_bytes=48 * 1024 * 1024
        ),
        name="relay",
    )(
        pending[0],
        admissible,
        plan,
        vanished_hop,
        jnp.moveaxis(w_in[0], 1, 0),
        w_out[0],
        gain,
    )
    return out[None], standby[None]


def solution(mesh):
    placed = (
        P("section", None, None),
        P(None, None, "tp"),
        P(),
        P(),
        P("section", None, None, "tp"),
        P("section", "tp", None),
        P("section", None),
    )
    return jax.shard_map(
        per_device,
        mesh=mesh,
        in_specs=placed,
        out_specs=(P("section", None, None), P("section", None, "tp")),
        check_vma=False,
    )
```

```python
import functools

import jax
import jax.numpy as jnp
from jax import lax
from jax.experimental import pallas as pl
from jax.experimental.pallas import tpu as pltpu
from jax.sharding import PartitionSpec as P

HD = 128
LANES = 128
SLOTS = 5
CHUNKS = 2
NORM_EPS = 1e-05
MESH = pl.DeviceIdType.MESH


def arrive(ref, sem):
    pltpu.make_async_copy(ref, ref, sem).wait()


def kernel(
    side,
    pending,
    admissible_hbm,
    plan_hbm,
    vanished,
    w_in_hbm,
    w_out_hbm,
    gain_hbm,
    out_ref,
    standby_ref,
    x_raw,
    w_in,
    w_out,
    x,
    ctx,
    y_real,
    y_send,
    normed,
    keys,
    values,
    spare,
    admissible,
    gain,
    plan,
    load_sem,
    wo_sem,
    ctx_sem,
    one_sem,
    two_sem,
    end_sem,
):
    sections = lax.axis_size("section")
    section = lax.axis_index("section")
    tp = lax.axis_index("tp")
    count = side * side
    z, y = tp // side, tp % side
    following = (section + 1) % sections
    final = sections - 1
    rows, width = pending.shape[0], pending.shape[1]
    part = rows // CHUNKS
    cols = width // count
    halves = cols // LANES

    def send(src, dst, sems, where):
        copy = pltpu.make_async_remote_copy(
            src_ref=src,
            dst_ref=dst,
            send_sem=sems.at[0],
            recv_sem=sems.at[1],
            device_id=where,
            device_id_type=MESH,
        )
        copy.start()

    def others(dz, dy):
        return ((z + dz) % side) * side + (y + dy) % side

    steps = sorted(
        ((a, b) for a in range(side) for b in range(side) if a or b),
        key=lambda s: -sum(min(d, side - d) for d in s),
    )

    barrier = pltpu.get_barrier_semaphore()
    before = (section + final) % sections
    senders = [(section, others(dz, dy)) for dz, dy in steps]
    senders += [(before, others(d, 0)) for d in range(side)]
    senders += [(before, others(0, d)) for d in range(1, side)]
    for sender in senders:
        pl.semaphore_signal(barrier, inc=1, device_id=sender, device_id_type=MESH)
    smalls = [
        pltpu.make_async_copy(src, dst, load_sem.at[5 + i])
        for i, (src, dst) in enumerate(
            ((plan_hbm, plan), (gain_hbm, gain), (admissible_hbm, admissible))
        )
    ]
    for load in smalls:
        load.start()

    load_x = pltpu.make_async_copy(pending, x_raw, load_sem.at[0])
    load_x.start()
    loads = [
        pltpu.make_async_copy(
            w_in_hbm.at[j], w_in.at[:, pl.ds(j * HD, HD)], load_sem.at[1 + j]
        )
        for j in range(3)
    ]
    for load in loads:
        load.start()
    own = pltpu.make_async_copy(
        w_out_hbm.at[:, pl.ds(pl.multiple_of(tp * cols, LANES), cols)], w_out.at[tp], load_sem.at[4]
    )
    own.start()
    pl.semaphore_wait(barrier, len(senders))
    for dz, dy in steps:
        peer = others(dz, dy)
        send(
            w_out_hbm.at[:, pl.ds(pl.multiple_of(peer * cols, LANES), cols)],
            w_out.at[tp],
            wo_sem,
            (section, peer),
        )
    for load in smalls:
        load.wait()
    lost = vanished[0]
    late_wrap = (lost == final - 1) | (lost == final - 2)
    load_x.wait()
    for c in range(count):
        for h in range(halves):
            for r in range(CHUNKS):
                block = x_raw[r * part : (r + 1) * part, c * cols + h * LANES : c * cols + (h + 1) * LANES]
                x[0, r, h, c // side, c % side] = jnp.where(section == lost, jnp.zeros_like(block), block)
    for load in loads:
        load.wait()

    def heads(k, r):
        def blocks():
            for c in range(count):
                for h in range(halves):
                    yield c * cols + h * LANES, x[k, r, h, c // side, c % side].astype(jnp.float32)

        total = jnp.zeros((part, LANES), jnp.float32)
        for _, block in blocks():
            total = total + block
        mean = jnp.sum(total, axis=-1, keepdims=True) * (1.0 / width)
        total = jnp.zeros((part, LANES), jnp.float32)
        for _, block in blocks():
            block = block - mean
            total = total + block * block
        scale = lax.rsqrt(jnp.sum(total, axis=-1, keepdims=True) * (1.0 / width) + NORM_EPS)
        for at, block in blocks():
            g = gain[:, at : at + LANES].astype(jnp.float32)
            normed[:, at : at + LANES] = ((block - mean) * scale * g).astype(jnp.bfloat16)
        projected = jnp.dot(normed[...], w_in[...], preferred_element_type=jnp.float32).astype(
            jnp.bfloat16
        )
        keys[r * part : (r + 1) * part, :] = projected[:, HD : 2 * HD]
        values[r * part : (r + 1) * part, :] = projected[:, 2 * HD :]
        seen = (r + 1) * part
        scores = lax.dot_general(
            projected[:, :HD],
            keys[:seen, :],
            (((1,), (1,)), ((), ())),
            preferred_element_type=jnp.float32,
        ) * HD ** (-0.5)
        row = lax.broadcasted_iota(jnp.int32, (part, seen), 0) + r * part
        col = lax.broadcasted_iota(jnp.int32, (part, seen), 1)
        scores = jnp.where(row >= col, scores, -jnp.inf)
        weights = jnp.exp(scores - jnp.max(scores, axis=-1, keepdims=True))
        probs = (weights / jnp.sum(weights, axis=-1, keepdims=True)).astype(jnp.bfloat16)
        mixed = jnp.dot(probs, values[:seen, :], preferred_element_type=jnp.float32)
        ctx[k, r, tp] = mixed.astype(jnp.bfloat16)
        for dz, dy in steps:
            send(ctx.at[k, r, tp], ctx.at[k, r, tp], ctx_sem.at[k, r], (section, others(dz, dy)))

    def mix(k, r):
        arrive(ctx.at[k, r, pl.ds(0, count - 1)], ctx_sem.at[k, r, 1])
        context = jnp.concatenate([ctx[k, r, i] for i in range(count)], axis=1)
        weights = w_out[...].reshape(count * HD, cols)
        branch = jnp.dot(context, weights, preferred_element_type=jnp.float32)
        mine = jnp.concatenate([x[k, r, h, z, y] for h in range(halves)], axis=1)
        result = (mine.astype(jnp.float32) + branch).astype(jnp.bfloat16)
        y_real[k, r] = result

        @pl.when(k < SLOTS - 1)
        def _():
            entering = admissible[plan[jnp.minimum(k, 2)], r * part : (r + 1) * part, :]
            enters = (k < 2) | ((k == 2) & late_wrap) | ((k == 3) & jnp.logical_not(late_wrap))
            held = jnp.where((k == 2) & (lost == final), y_real[0, r], result)
            wrapped = jnp.where(enters, entering, held)
            sent = jnp.where(section == final, wrapped, result)
            for h in range(halves):
                y_send[k, r, h] = sent[:, h * LANES : (h + 1) * LANES]
                for step in range(side):
                    peer = others(step, 0) if h == 0 else others(0, step)
                    send(
                        y_send.at[k, r, h],
                        x.at[k + 1, r, h, z, y],
                        one_sem.at[k, r, h],
                        (following, peer),
                    )

    def line(k, r, h):
        return x.at[k + 1, r, h, :, y] if h == 0 else x.at[k + 1, r, h, z]

    def forward(k, r):
        for h in range(halves):
            arrive(x.at[k + 1, r, h, 0], one_sem.at[k, r, h, 1])
            for step in range(1, side):
                peer = others(0, step) if h == 0 else others(step, 0)
                send(line(k, r, h), line(k, r, h), two_sem.at[k, r, h], (section, peer))

    def gathered(k, r):
        for h in range(halves):
            arrive(x.at[k + 1, r, h, pl.ds(0, side - 1)], two_sem.at[k, r, h, 1])

    def slot(k, carry):
        for r in range(CHUNKS):

            @pl.when(k > 0)
            def _():
                gathered(k - 1, r)

            heads(k, r)

        @pl.when(k == 0)
        def _():
            own.wait()
            arrive(w_out.at[pl.ds(0, count - 1)], wo_sem.at[1])

        @pl.when(k == SLOTS - 1)
        def _():
            behind = (section > lost) & (section <= lost + 3)
            newest = jnp.where(section == 0, jnp.logical_not(late_wrap), behind)
            for c in range(count):
                for h in range(halves):
                    for r in range(CHUNKS):
                        at = (r, h, c // side, c % side)
                        block = jnp.where(newest, x[SLOTS - 1, *at], x[SLOTS - 2, *at])
                        block = jnp.where(section == lost, jnp.zeros_like(block), block)
                        start = c * cols + h * LANES
                        out_ref[r * part : (r + 1) * part, start : start + LANES] = block

        for r in range(CHUNKS):
            mix(k, r)

        @pl.when(k < SLOTS - 1)
        def _():
            for r in range(CHUNKS):
                forward(k, r)

        return carry

    lax.fori_loop(0, SLOTS, slot, 0)

    target = (section + 1) % sections
    early = (target == (lost + 2) % sections) & (lost <= final - 1)
    late = ((target == (lost + 3) % sections) & (lost <= final - 1)) | (
        (target == (lost + 4) % sections) & (lost <= final - 2)
    )
    for r in range(CHUNKS):
        chosen = jnp.where(early, y_real[1, r], jnp.where(late, y_real[4, r], y_real[3, r]))
        spare[r] = chosen
        send(spare.at[r], standby_ref.at[pl.ds(r * part, part)], end_sem.at[r], (following, tp))

    arrive(w_out.at[pl.ds(0, count - 1)], wo_sem.at[0])

    def drain(k, carry):
        for r in range(CHUNKS):
            arrive(ctx.at[k, r, pl.ds(0, count - 1)], ctx_sem.at[k, r, 0])

            @pl.when(k < SLOTS - 1)
            def _():
                for h in range(halves):
                    arrive(x.at[k, r, h, 0], one_sem.at[k, r, h, 0])
                    arrive(x.at[k, r, h, pl.ds(0, side - 1)], two_sem.at[k, r, h, 0])

        return carry

    lax.fori_loop(0, SLOTS, drain, 0)
    for r in range(CHUNKS):
        arrive(spare.at[r], end_sem.at[r, 0])
        arrive(spare.at[r], end_sem.at[r, 1])


def in_hbm(array):
    return pltpu.with_memory_space_constraint(array, pltpu.HBM)


def per_device(pending, admissible, plan, vanished_hop, w_in, w_out, gain):
    count = lax.axis_size("tp")
    side = int(round(count**0.5))
    rows, width = pending.shape[1:]
    cols = width // count
    part = rows // CHUNKS
    halves = cols // LANES
    vmem = pl.BlockSpec(memory_space=pltpu.VMEM)
    smem = pl.BlockSpec(memory_space=pltpu.SMEM)
    hbm = pl.BlockSpec(memory_space=pltpu.HBM)
    bf16 = jnp.bfloat16
    dma = pltpu.SemaphoreType.DMA
    out, standby = pl.pallas_call(
        functools.partial(kernel, side),
        out_shape=(
            jax.ShapeDtypeStruct((rows, width), bf16),
            jax.ShapeDtypeStruct((rows, cols), bf16),
        ),
        in_specs=[hbm] * 3 + [smem] + [hbm] * 3,
        out_specs=(vmem, vmem),
        scratch_shapes=[
            pltpu.VMEM((rows, width), bf16),
            pltpu.VMEM((width, 3 * HD), bf16),
            pltpu.VMEM((count, HD, cols), bf16),
            pltpu.VMEM((SLOTS, CHUNKS, halves, side, side, part, LANES), bf16),
            pltpu.VMEM((SLOTS, CHUNKS, count, part, HD), bf16),
            pltpu.VMEM((SLOTS, CHUNKS, part, cols), bf16),
            pltpu.VMEM((SLOTS - 1, CHUNKS, halves, part, LANES), bf16),
            pltpu.VMEM((part, width), bf16),
            pltpu.VMEM((rows, HD), bf16),
            pltpu.VMEM((rows, HD), bf16),
            pltpu.VMEM((CHUNKS, part, cols), bf16),
            pltpu.VMEM(admissible.shape, bf16),
            pltpu.VMEM(gain.shape, bf16),
            pltpu.SMEM(plan.shape, jnp.int32),
            dma((8,)),
            dma((2,)),
            dma((SLOTS, CHUNKS, 2)),
            dma((SLOTS - 1, CHUNKS, halves, 2)),
            dma((SLOTS - 1, CHUNKS, halves, 2)),
            dma((CHUNKS, 2)),
        ],
        compiler_params=pltpu.CompilerParams(
            has_side_effects=True, vmem_limit_bytes=48 * 1024 * 1024, collective_id=0
        ),
        name="relay",
    )(
        in_hbm(pending[0]),
        in_hbm(admissible),
        in_hbm(plan),
        vanished_hop,
        in_hbm(jnp.moveaxis(w_in[0], 1, 0)),
        in_hbm(w_out[0]),
        in_hbm(gain),
    )
    return out[None], standby[None]


def solution(mesh):
    placed = (
        P("section", None, None),
        P(None, None, "tp"),
        P(),
        P(),
        P("section", None, None, "tp"),
        P("section", "tp", None),
        P("section", None),
    )
    return jax.shard_map(
        per_device,
        mesh=mesh,
        in_specs=placed,
        out_specs=(P("section", None, None), P("section", None, "tp")),
        check_vma=False,
    )
```

```python
import functools

import jax
import jax.numpy as jnp
from jax import lax
from jax.experimental import pallas as pl
from jax.experimental.pallas import tpu as pltpu
from jax.sharding import PartitionSpec as P

HD = 128
LANES = 128
SLOTS = 5
CHUNKS = 4
NORM_EPS = 1e-05
MESH = pl.DeviceIdType.MESH


def arrive(ref, sem):
    pltpu.make_async_copy(ref, ref, sem).wait()


def kernel(
    side,
    pending,
    admissible_hbm,
    plan_hbm,
    vanished,
    w_in_hbm,
    w_out_hbm,
    gain_hbm,
    out_ref,
    standby_ref,
    x_raw,
    w_in,
    w_out,
    x,
    ctx,
    y_real,
    y_send,
    normed,
    keys,
    values,
    spare,
    admissible,
    gain,
    plan,
    load_sem,
    wo_sem,
    ctx_sem,
    one_sem,
    two_sem,
    end_sem,
):
    sections = lax.axis_size("section")
    section = lax.axis_index("section")
    tp = lax.axis_index("tp")
    count = side * side
    z, y = tp // side, tp % side
    following = (section + 1) % sections
    final = sections - 1
    rows, width = pending.shape[0], pending.shape[1]
    part = rows // CHUNKS
    cols = width // count
    halves = cols // LANES

    def send(src, dst, sems, where):
        copy = pltpu.make_async_remote_copy(
            src_ref=src,
            dst_ref=dst,
            send_sem=sems.at[0],
            recv_sem=sems.at[1],
            device_id=where,
            device_id_type=MESH,
        )
        copy.start()

    def others(dz, dy):
        return ((z + dz) % side) * side + (y + dy) % side

    steps = sorted(
        ((a, b) for a in range(side) for b in range(side) if a or b),
        key=lambda s: -sum(min(d, side - d) for d in s),
    )

    barrier = pltpu.get_barrier_semaphore()
    before = (section + final) % sections
    senders = [(section, others(dz, dy)) for dz, dy in steps]
    senders += [(before, others(d, 0)) for d in range(side)]
    senders += [(before, others(0, d)) for d in range(1, side)]
    for sender in senders:
        pl.semaphore_signal(barrier, inc=1, device_id=sender, device_id_type=MESH)
    smalls = [
        pltpu.make_async_copy(src, dst, load_sem.at[5 + i])
        for i, (src, dst) in enumerate(
            ((plan_hbm, plan), (gain_hbm, gain), (admissible_hbm, admissible))
        )
    ]
    for load in smalls:
        load.start()

    load_x = pltpu.make_async_copy(pending, x_raw, load_sem.at[0])
    load_x.start()
    loads = [
        pltpu.make_async_copy(
            w_in_hbm.at[j], w_in.at[:, pl.ds(j * HD, HD)], load_sem.at[1 + j]
        )
        for j in range(3)
    ]
    for load in loads:
        load.start()
    own = pltpu.make_async_copy(
        w_out_hbm.at[:, pl.ds(pl.multiple_of(tp * cols, LANES), cols)], w_out.at[tp], load_sem.at[4]
    )
    own.start()
    pl.semaphore_wait(barrier, len(senders))
    for dz, dy in steps:
        peer = others(dz, dy)
        send(
            w_out_hbm.at[:, pl.ds(pl.multiple_of(peer * cols, LANES), cols)],
            w_out.at[tp],
            wo_sem,
            (section, peer),
        )
    for load in smalls:
        load.wait()
    lost = vanished[0]
    late_wrap = (lost == final - 1) | (lost == final - 2)
    load_x.wait()
    for c in range(count):
        for h in range(halves):
            for r in range(CHUNKS):
                block = x_raw[r * part : (r + 1) * part, c * cols + h * LANES : c * cols + (h + 1) * LANES]
                x[0, r, h, c // side, c % side] = jnp.where(section == lost, jnp.zeros_like(block), block)
    for load in loads:
        load.wait()

    def heads(k, r):
        def blocks():
            for c in range(count):
                for h in range(halves):
                    yield c * cols + h * LANES, x[k, r, h, c // side, c % side].astype(jnp.float32)

        total = jnp.zeros((part, LANES), jnp.float32)
        for _, block in blocks():
            total = total + block
        mean = jnp.sum(total, axis=-1, keepdims=True) * (1.0 / width)
        total = jnp.zeros((part, LANES), jnp.float32)
        for _, block in blocks():
            block = block - mean
            total = total + block * block
        scale = lax.rsqrt(jnp.sum(total, axis=-1, keepdims=True) * (1.0 / width) + NORM_EPS)
        for at, block in blocks():
            g = gain[:, at : at + LANES].astype(jnp.float32)
            normed[:, at : at + LANES] = ((block - mean) * scale * g).astype(jnp.bfloat16)
        projected = jnp.dot(normed[...], w_in[...], preferred_element_type=jnp.float32).astype(
            jnp.bfloat16
        )
        keys[r * part : (r + 1) * part, :] = projected[:, HD : 2 * HD]
        values[r * part : (r + 1) * part, :] = projected[:, 2 * HD :]
        seen = (r + 1) * part
        scores = lax.dot_general(
            projected[:, :HD],
            keys[:seen, :],
            (((1,), (1,)), ((), ())),
            preferred_element_type=jnp.float32,
        ) * HD ** (-0.5)
        row = lax.broadcasted_iota(jnp.int32, (part, seen), 0) + r * part
        col = lax.broadcasted_iota(jnp.int32, (part, seen), 1)
        scores = jnp.where(row >= col, scores, -jnp.inf)
        weights = jnp.exp(scores - jnp.max(scores, axis=-1, keepdims=True))
        probs = (weights / jnp.sum(weights, axis=-1, keepdims=True)).astype(jnp.bfloat16)
        mixed = jnp.dot(probs, values[:seen, :], preferred_element_type=jnp.float32)
        ctx[k, r, tp] = mixed.astype(jnp.bfloat16)
        for dz, dy in steps:
            send(ctx.at[k, r, tp], ctx.at[k, r, tp], ctx_sem.at[k, r], (section, others(dz, dy)))

    def mix(k, r):
        arrive(ctx.at[k, r, pl.ds(0, count - 1)], ctx_sem.at[k, r, 1])
        context = jnp.concatenate([ctx[k, r, i] for i in range(count)], axis=1)
        weights = w_out[...].reshape(count * HD, cols)
        branch = jnp.dot(context, weights, preferred_element_type=jnp.float32)
        mine = jnp.concatenate([x[k, r, h, z, y] for h in range(halves)], axis=1)
        result = (mine.astype(jnp.float32) + branch).astype(jnp.bfloat16)
        y_real[k, r] = result

        @pl.when(k < SLOTS - 1)
        def _():
            entering = admissible[plan[jnp.minimum(k, 2)], r * part : (r + 1) * part, :]
            enters = (k < 2) | ((k == 2) & late_wrap) | ((k == 3) & jnp.logical_not(late_wrap))
            held = jnp.where((k == 2) & (lost == final), y_real[0, r], result)
            wrapped = jnp.where(enters, entering, held)
            sent = jnp.where(section == final, wrapped, result)
            for h in range(halves):
                y_send[k, r, h] = sent[:, h * LANES : (h + 1) * LANES]
                for step in range(side):
                    peer = others(step, 0) if h == 0 else others(0, step)
                    send(
                        y_send.at[k, r, h],
                        x.at[k + 1, r, h, z, y],
                        one_sem.at[k, r, h],
                        (following, peer),
                    )

    def line(k, r, h):
        return x.at[k + 1, r, h, :, y] if h == 0 else x.at[k + 1, r, h, z]

    def forward(k, r):
        for h in range(halves):
            arrive(x.at[k + 1, r, h, 0], one_sem.at[k, r, h, 1])
            for step in range(1, side):
                peer = others(0, step) if h == 0 else others(step, 0)
                send(line(k, r, h), line(k, r, h), two_sem.at[k, r, h], (section, peer))

    def gathered(k, r):
        for h in range(halves):
            arrive(x.at[k + 1, r, h, pl.ds(0, side - 1)], two_sem.at[k, r, h, 1])

    def left(k):
        for r in range(CHUNKS):
            arrive(ctx.at[k, r, pl.ds(0, count - 1)], ctx_sem.at[k, r, 0])
            for h in range(halves):
                arrive(x.at[k, r, h, 0], one_sem.at[k, r, h, 0])
                arrive(x.at[k, r, h, pl.ds(0, side - 1)], two_sem.at[k, r, h, 0])

    def slot(k, carry):
        for r in range(CHUNKS):

            @pl.when(k > 0)
            def _():
                gathered(k - 1, r)

            heads(k, r)

        @pl.when(k == 0)
        def _():
            own.wait()
            arrive(w_out.at[pl.ds(0, count - 1)], wo_sem.at[1])

        @pl.when(k == SLOTS - 1)
        def _():
            arrive(w_out.at[pl.ds(0, count - 1)], wo_sem.at[0])
            behind = (section > lost) & (section <= lost + 3)
            newest = jnp.where(section == 0, jnp.logical_not(late_wrap), behind)
            for c in range(count):
                for h in range(halves):
                    for r in range(CHUNKS):
                        at = (r, h, c // side, c % side)
                        block = jnp.where(newest, x[SLOTS - 1, *at], x[SLOTS - 2, *at])
                        block = jnp.where(section == lost, jnp.zeros_like(block), block)
                        start = c * cols + h * LANES
                        out_ref[r * part : (r + 1) * part, start : start + LANES] = block

        @pl.when(k > 0)
        def _():
            left(k - 1)

        for r in range(CHUNKS - 1):
            mix(k, r)

        @pl.when(k < SLOTS - 1)
        def _():
            forward(k, 0)

        mix(k, CHUNKS - 1)

        @pl.when(k < SLOTS - 1)
        def _():
            for r in range(1, CHUNKS):
                forward(k, r)

        return carry

    lax.fori_loop(0, SLOTS, slot, 0)

    target = (section + 1) % sections
    early = (target == (lost + 2) % sections) & (lost <= final - 1)
    late = ((target == (lost + 3) % sections) & (lost <= final - 1)) | (
        (target == (lost + 4) % sections) & (lost <= final - 2)
    )
    for r in range(CHUNKS):
        chosen = jnp.where(early, y_real[1, r], jnp.where(late, y_real[4, r], y_real[3, r]))
        spare[r] = chosen
        send(spare.at[r], standby_ref.at[pl.ds(r * part, part)], end_sem.at[r], (following, tp))

    for r in range(CHUNKS):
        arrive(ctx.at[SLOTS - 1, r, pl.ds(0, count - 1)], ctx_sem.at[SLOTS - 1, r, 0])
    for r in range(CHUNKS):
        arrive(spare.at[r], end_sem.at[r, 0])
        arrive(spare.at[r], end_sem.at[r, 1])


def in_hbm(array):
    return pltpu.with_memory_space_constraint(array, pltpu.HBM)


def per_device(pending, admissible, plan, vanished_hop, w_in, w_out, gain):
    count = lax.axis_size("tp")
    side = int(round(count**0.5))
    rows, width = pending.shape[1:]
    cols = width // count
    part = rows // CHUNKS
    halves = cols // LANES
    vmem = pl.BlockSpec(memory_space=pltpu.VMEM)
    smem = pl.BlockSpec(memory_space=pltpu.SMEM)
    hbm = pl.BlockSpec(memory_space=pltpu.HBM)
    bf16 = jnp.bfloat16
    dma = pltpu.SemaphoreType.DMA
    out, standby = pl.pallas_call(
        functools.partial(kernel, side),
        out_shape=(
            jax.ShapeDtypeStruct((rows, width), bf16),
            jax.ShapeDtypeStruct((rows, cols), bf16),
        ),
        in_specs=[hbm] * 3 + [smem] + [hbm] * 3,
        out_specs=(vmem, vmem),
        scratch_shapes=[
            pltpu.VMEM((rows, width), bf16),
            pltpu.VMEM((width, 3 * HD), bf16),
            pltpu.VMEM((count, HD, cols), bf16),
            pltpu.VMEM((SLOTS, CHUNKS, halves, side, side, part, LANES), bf16),
            pltpu.VMEM((SLOTS, CHUNKS, count, part, HD), bf16),
            pltpu.VMEM((SLOTS, CHUNKS, part, cols), bf16),
            pltpu.VMEM((SLOTS - 1, CHUNKS, halves, part, LANES), bf16),
            pltpu.VMEM((part, width), bf16),
            pltpu.VMEM((rows, HD), bf16),
            pltpu.VMEM((rows, HD), bf16),
            pltpu.VMEM((CHUNKS, part, cols), bf16),
            pltpu.VMEM(admissible.shape, bf16),
            pltpu.VMEM(gain.shape, bf16),
            pltpu.SMEM(plan.shape, jnp.int32),
            dma((8,)),
            dma((2,)),
            dma((SLOTS, CHUNKS, 2)),
            dma((SLOTS - 1, CHUNKS, halves, 2)),
            dma((SLOTS - 1, CHUNKS, halves, 2)),
            dma((CHUNKS, 2)),
        ],
        compiler_params=pltpu.CompilerParams(
            has_side_effects=True, vmem_limit_bytes=48 * 1024 * 1024, collective_id=0
        ),
        name="relay",
    )(
        in_hbm(pending[0]),
        in_hbm(admissible),
        in_hbm(plan),
        vanished_hop,
        in_hbm(jnp.moveaxis(w_in[0], 1, 0)),
        in_hbm(w_out[0]),
        in_hbm(gain),
    )
    return out[None], standby[None]


def solution(mesh):
    placed = (
        P("section", None, None),
        P(None, None, "tp"),
        P(),
        P(),
        P("section", None, None, "tp"),
        P("section", "tp", None),
        P("section", None),
    )
    return jax.shard_map(
        per_device,
        mesh=mesh,
        in_specs=placed,
        out_specs=(P("section", None, None), P("section", None, "tp")),
        check_vma=False,
    )
```

```python
import functools

import jax
import jax.numpy as jnp
from jax import lax
from jax.experimental import pallas as pl
from jax.experimental.pallas import tpu as pltpu
from jax.sharding import PartitionSpec as P

HD = 128
LANES = 128
SLOTS = 5
CHUNKS = 4
NORM_EPS = 1e-05
MESH = pl.DeviceIdType.MESH


def arrive(ref, sem):
    pltpu.make_async_copy(ref, ref, sem).wait()


def kernel(
    side,
    pending,
    admissible_hbm,
    plan_hbm,
    vanished,
    w_in_hbm,
    w_out_hbm,
    gain_hbm,
    out_ref,
    standby_ref,
    x_raw,
    w_in,
    w_line,
    x,
    ctx,
    kept,
    sent,
    got,
    total,
    normed,
    keys,
    values,
    spare,
    spare_got,
    admissible,
    gain,
    plan,
    load_sem,
    wo_sem,
    ctx_sem,
    part_sem,
    sum_sem,
    end_sem,
):
    sections = lax.axis_size("section")
    section = lax.axis_index("section")
    tp = lax.axis_index("tp")
    count = side * side
    z, y = tp // side, tp % side
    place = (z, y)
    final = sections - 1
    following = (section + 1) % sections
    before = (section + final) % sections
    rows, width = pending.shape[0], pending.shape[1]
    part = rows // CHUNKS
    cols = width // count
    halves = cols // LANES

    def send(src, dst, sems, where):
        copy = pltpu.make_async_remote_copy(
            src_ref=src,
            dst_ref=dst,
            send_sem=sems.at[0],
            recv_sem=sems.at[1],
            device_id=where,
            device_id_type=MESH,
        )
        copy.start()

    def on_line(line, step):
        if line == 0:
            return ((z + step) % side) * side + y
        return z * side + (y + step) % side

    far_first = [2, 1, 3] if side == 4 else list(range(1, side))

    barrier = pltpu.get_barrier_semaphore()
    senders = [(section, on_line(line, d)) for line in range(2) for d in range(1, side)]
    senders += [(before, on_line(0, d)) for d in range(side)]
    senders += [(before, on_line(1, d)) for d in range(1, side)]
    for sender in senders:
        pl.semaphore_signal(barrier, inc=1, device_id=sender, device_id_type=MESH)
    smalls = [
        pltpu.make_async_copy(src, dst, load_sem.at[6 + i])
        for i, (src, dst) in enumerate(
            ((plan_hbm, plan), (gain_hbm, gain), (admissible_hbm, admissible))
        )
    ]
    for load in smalls:
        load.start()
    load_x = pltpu.make_async_copy(pending, x_raw, load_sem.at[0])
    load_x.start()
    loads = [
        pltpu.make_async_copy(
            w_in_hbm.at[j], w_in.at[:, pl.ds(j * HD, HD)], load_sem.at[1 + j]
        )
        for j in range(3)
    ]
    for load in loads:
        load.start()

    def columns(line, peer_at, q):
        block = peer_at * side + q if line == 0 else q * side + peer_at
        return w_out_hbm.at[:, pl.ds(pl.multiple_of(block * cols + line * LANES, LANES), LANES)]

    for line in range(2):
        for q in range(side):
            pltpu.make_async_copy(
                columns(line, place[line], q),
                w_line.at[line, place[line], :, pl.ds(q * LANES, LANES)],
                load_sem.at[4 + line],
            ).start()
    pl.semaphore_wait(barrier, len(senders))
    for step in far_first:
        for line in range(2):
            for q in range(side):
                send(
                    columns(line, (place[line] + step) % side, q),
                    w_line.at[line, place[line], :, pl.ds(q * LANES, LANES)],
                    wo_sem.at[line],
                    (section, on_line(line, step)),
                )
    for load in smalls:
        load.wait()
    lost = vanished[0]
    late_wrap = (lost == final - 1) | (lost == final - 2)
    load_x.wait()
    for c in range(count):
        for h in range(halves):
            for r in range(CHUNKS):
                start = c * cols + h * LANES
                block = x_raw[r * part : (r + 1) * part, start : start + LANES]
                x[0, r, h, c // side, c % side] = jnp.where(
                    section == lost, jnp.zeros_like(block), block
                )
    for load in loads:
        load.wait()

    def heads(k, r):
        def blocks():
            for c in range(count):
                for h in range(halves):
                    yield c * cols + h * LANES, x[k, r, h, c // side, c % side].astype(jnp.float32)

        summed = jnp.zeros((part, LANES), jnp.float32)
        for _, block in blocks():
            summed = summed + block
        mean = jnp.sum(summed, axis=-1, keepdims=True) * (1.0 / width)
        summed = jnp.zeros((part, LANES), jnp.float32)
        for _, block in blocks():
            block = block - mean
            summed = summed + block * block
        scale = lax.rsqrt(jnp.sum(summed, axis=-1, keepdims=True) * (1.0 / width) + NORM_EPS)
        for at, block in blocks():
            g = gain[:, at : at + LANES].astype(jnp.float32)
            normed[:, at : at + LANES] = ((block - mean) * scale * g).astype(jnp.bfloat16)
        projected = jnp.dot(normed[...], w_in[...], preferred_element_type=jnp.float32).astype(
            jnp.bfloat16
        )
        keys[r * part : (r + 1) * part, :] = projected[:, HD : 2 * HD]
        values[r * part : (r + 1) * part, :] = projected[:, 2 * HD :]
        seen = (r + 1) * part
        scores = lax.dot_general(
            projected[:, :HD],
            keys[:seen, :],
            (((1,), (1,)), ((), ())),
            preferred_element_type=jnp.float32,
        ) * HD ** (-0.5)
        row = lax.broadcasted_iota(jnp.int32, (part, seen), 0) + r * part
        col = lax.broadcasted_iota(jnp.int32, (part, seen), 1)
        scores = jnp.where(row >= col, scores, -jnp.inf)
        weights = jnp.exp(scores - jnp.max(scores, axis=-1, keepdims=True))
        probs = (weights / jnp.sum(weights, axis=-1, keepdims=True)).astype(jnp.bfloat16)
        mixed = jnp.dot(probs, values[:seen, :], preferred_element_type=jnp.float32)
        mixed = mixed.astype(jnp.bfloat16)
        for line in range(2):
            ctx[k, r, line, place[line]] = mixed
        for step in far_first:
            for line in range(2):
                block = ctx.at[k, r, line, place[line]]
                send(block, block, ctx_sem.at[k, r, line], (section, on_line(line, step)))

    def mix(k, r):
        early = (following == (lost + 2) % sections) & (lost <= final - 1)
        late = ((following == (lost + 3) % sections) & (lost <= final - 1)) | (
            (following == (lost + 4) % sections) & (lost <= final - 2)
        )
        enters = (k < 2) | ((k == 2) & late_wrap) | ((k == 3) & jnp.logical_not(late_wrap))
        enters = enters & (section == final)
        holds = (k == 2) & (lost == final) & (section == final)
        for line in range(2):
            arrive(ctx.at[k, r, line, pl.ds(0, side - 1)], ctx_sem.at[k, r, line, 1])
            context = jnp.concatenate([ctx[k, r, line, i] for i in range(side)], axis=1)
            branch = jnp.dot(
                context,
                w_line[line].reshape(side * HD, side * LANES),
                preferred_element_type=jnp.float32,
            )
            across = place[1 - line]
            for q in range(side):
                block = x[k, r, 0, z, q] if line == 0 else x[k, r, 1, q, y]
                share = branch[:, q * LANES : (q + 1) * LANES] + jnp.where(
                    across == q, block.astype(jnp.float32), 0.0
                )
                kept[k, r, line, q] = share.astype(jnp.bfloat16)

            @pl.when(k < SLOTS - 1)
            def _():
                entering = admissible[
                    plan[jnp.minimum(k, 2)],
                    r * part : (r + 1) * part,
                    line * LANES : (line + 1) * LANES,
                ]
                for q in range(side):
                    fresh = jnp.where(across == q, entering, jnp.zeros_like(entering))
                    value = jnp.where(holds, kept[0, r, line, q], kept[k, r, line, q])
                    sent[k, r, line, q] = jnp.where(enters, fresh, value)
                if line == 0:
                    for step in [*far_first, 0]:
                        send(
                            sent.at[k, r, 0],
                            got.at[k, r, 0, y],
                            part_sem.at[k, r, 0],
                            (following, on_line(1, step)),
                        )
                else:
                    for step in far_first:
                        send(
                            sent.at[k, r, 1],
                            got.at[k, r, 1, z],
                            part_sem.at[k, r, 1],
                            (section, on_line(0, step)),
                        )
                    for q in range(side):
                        got[k, r, 1, z, q] = sent[k, r, 1, q]

            @pl.when(k == SLOTS - 1)
            def _():
                for q in range(side):
                    value = jnp.where(late, kept[k, r, line, q], kept[3, r, line, q])
                    spare[r, line, q] = jnp.where(early, kept[1, r, line, q], value)
                for q in range(side):
                    send(
                        spare.at[r, line, q],
                        spare_got.at[r, line, across],
                        end_sem.at[r, line],
                        (following, z * side + q if line == 0 else q * side + y),
                    )

    def summed(k, r, line, q):
        value = got[k, r, line, 0, q].astype(jnp.float32)
        for i in range(1, side):
            value = value + got[k, r, line, i, q].astype(jnp.float32)
        return value.astype(jnp.bfloat16)

    def forward(k, r):
        arrive(got.at[k, r, 0], part_sem.at[k, r, 0, 1])
        for q in range(side):
            x[k + 1, r, 0, z, q] = summed(k, r, 0, q)
        for step in far_first:
            block = x.at[k + 1, r, 0, z]
            send(block, block, sum_sem.at[k, r, 0], (section, on_line(0, step)))
        arrive(got.at[k, r, 1, pl.ds(0, side - 1)], part_sem.at[k, r, 1, 1])
        for q in range(side):
            total[k, r, q] = summed(k, r, 1, q)
        for step in [*far_first, 0]:
            send(
                total.at[k, r],
                x.at[k + 1, r, 1, :, y],
                sum_sem.at[k, r, 1],
                (following, on_line(1, step)),
            )

    def gathered(k, r):
        arrive(x.at[k + 1, r, 0, pl.ds(0, side - 1)], sum_sem.at[k, r, 0, 1])
        arrive(x.at[k + 1, r, 1], sum_sem.at[k, r, 1, 1])

    def left(k):
        for r in range(CHUNKS):
            for line in range(2):
                arrive(ctx.at[k, r, line, pl.ds(0, side - 1)], ctx_sem.at[k, r, line, 0])
            arrive(got.at[k, r, 0], part_sem.at[k, r, 0, 0])
            arrive(got.at[k, r, 1, pl.ds(0, side - 1)], part_sem.at[k, r, 1, 0])
            arrive(x.at[k, r, 0, pl.ds(0, side - 1)], sum_sem.at[k, r, 0, 0])
            arrive(x.at[k, r, 1], sum_sem.at[k, r, 1, 0])

    def slot(k, carry):
        for r in range(CHUNKS):

            @pl.when(k > 0)
            def _():
                gathered(k - 1, r)

            heads(k, r)

        @pl.when(k == 0)
        def _():
            for line in range(2):
                arrive(w_line.at[line, 0], load_sem.at[4 + line])
                arrive(w_line.at[line, pl.ds(0, side - 1)], wo_sem.at[line, 1])

        @pl.when(k == SLOTS - 1)
        def _():
            for line in range(2):
                arrive(w_line.at[line, pl.ds(0, side - 1)], wo_sem.at[line, 0])
            behind = (section > lost) & (section <= lost + 3)
            newest = jnp.where(section == 0, jnp.logical_not(late_wrap), behind)
            for c in range(count):
                for h in range(halves):
                    for r in range(CHUNKS):
                        at = (r, h, c // side, c % side)
                        block = jnp.where(newest, x[SLOTS - 1, *at], x[SLOTS - 2, *at])
                        block = jnp.where(section == lost, jnp.zeros_like(block), block)
                        start = c * cols + h * LANES
                        out_ref[r * part : (r + 1) * part, start : start + LANES] = block

        @pl.when(k > 0)
        def _():
            left(k - 1)

        for r in range(CHUNKS):
            mix(k, r)

        @pl.when(k < SLOTS - 1)
        def _():
            for r in range(CHUNKS):
                forward(k, r)

        return carry

    lax.fori_loop(0, SLOTS, slot, 0)

    for r in range(CHUNKS):
        for line in range(2):
            arrive(spare_got.at[r, line], end_sem.at[r, line, 1])
            value = spare_got[r, line, 0].astype(jnp.float32)
            for i in range(1, side):
                value = value + spare_got[r, line, i].astype(jnp.float32)
            standby_ref[r * part : (r + 1) * part, line * LANES : (line + 1) * LANES] = (
                value.astype(jnp.bfloat16)
            )
    for r in range(CHUNKS):
        for line in range(2):
            arrive(ctx.at[SLOTS - 1, r, line, pl.ds(0, side - 1)], ctx_sem.at[SLOTS - 1, r, line, 0])
            arrive(spare.at[r, line], end_sem.at[r, line, 0])


def in_hbm(array):
    return pltpu.with_memory_space_constraint(array, pltpu.HBM)


def per_device(pending, admissible, plan, vanished_hop, w_in, w_out, gain):
    count = lax.axis_size("tp")
    side = int(round(count**0.5))
    rows, width = pending.shape[1:]
    cols = width // count
    part = rows // CHUNKS
    halves = cols // LANES
    vmem = pl.BlockSpec(memory_space=pltpu.VMEM)
    smem = pl.BlockSpec(memory_space=pltpu.SMEM)
    hbm = pl.BlockSpec(memory_space=pltpu.HBM)
    bf16 = jnp.bfloat16
    dma = pltpu.SemaphoreType.DMA
    out, standby = pl.pallas_call(
        functools.partial(kernel, side),
        out_shape=(
            jax.ShapeDtypeStruct((rows, width), bf16),
            jax.ShapeDtypeStruct((rows, cols), bf16),
        ),
        in_specs=[hbm] * 3 + [smem] + [hbm] * 3,
        out_specs=(vmem, vmem),
        scratch_shapes=[
            pltpu.VMEM((rows, width), bf16),
            pltpu.VMEM((width, 3 * HD), bf16),
            pltpu.VMEM((2, side, HD, side * LANES), bf16),
            pltpu.VMEM((SLOTS, CHUNKS, halves, side, side, part, LANES), bf16),
            pltpu.VMEM((SLOTS, CHUNKS, 2, side, part, HD), bf16),
            pltpu.VMEM((SLOTS, CHUNKS, 2, side, part, LANES), bf16),
            pltpu.VMEM((SLOTS - 1, CHUNKS, 2, side, part, LANES), bf16),
            pltpu.VMEM((SLOTS - 1, CHUNKS, 2, side, side, part, LANES), bf16),
            pltpu.VMEM((SLOTS - 1, CHUNKS, side, part, LANES), bf16),
            pltpu.VMEM((part, width), bf16),
            pltpu.VMEM((rows, HD), bf16),
            pltpu.VMEM((rows, HD), bf16),
            pltpu.VMEM((CHUNKS, 2, side, part, LANES), bf16),
            pltpu.VMEM((CHUNKS, 2, side, part, LANES), bf16),
            pltpu.VMEM(admissible.shape, bf16),
            pltpu.VMEM(gain.shape, bf16),
            pltpu.SMEM(plan.shape, jnp.int32),
            dma((9,)),
            dma((2, 2)),
            dma((SLOTS, CHUNKS, 2, 2)),
            dma((SLOTS - 1, CHUNKS, 2, 2)),
            dma((SLOTS - 1, CHUNKS, 2, 2)),
            dma((CHUNKS, 2, 2)),
        ],
        compiler_params=pltpu.CompilerParams(
            has_side_effects=True, vmem_limit_bytes=48 * 1024 * 1024, collective_id=0
        ),
        name="relay",
    )(
        in_hbm(pending[0]),
        in_hbm(admissible),
        in_hbm(plan),
        vanished_hop,
        in_hbm(jnp.moveaxis(w_in[0], 1, 0)),
        in_hbm(w_out[0]),
        in_hbm(gain),
    )
    return out[None], standby[None]


def solution(mesh):
    placed = (
        P("section", None, None),
        P(None, None, "tp"),
        P(),
        P(),
        P("section", None, None, "tp"),
        P("section", "tp", None),
        P("section", None),
    )
    return jax.shard_map(
        per_device,
        mesh=mesh,
        in_specs=placed,
        out_specs=(P("section", None, None), P("section", None, "tp")),
        check_vma=False,
    )
```

```python
import functools

import jax
import jax.numpy as jnp
from jax import lax
from jax.experimental import pallas as pl
from jax.experimental.pallas import tpu as pltpu
from jax.sharding import PartitionSpec as P

HD = 128
LANES = 128
SLOTS = 5
CHUNKS = 4
NORM_EPS = 1e-05
MESH = pl.DeviceIdType.MESH


def arrive(ref, sem):
    pltpu.make_async_copy(ref, ref, sem).wait()


def kernel(
    side,
    pending,
    admissible_hbm,
    plan_hbm,
    vanished,
    w_in_hbm,
    w_out_hbm,
    gain_hbm,
    out_ref,
    standby_ref,
    x_raw,
    w_in,
    w_line,
    x,
    ctx,
    kept,
    sent,
    got,
    total,
    normed,
    keys,
    values,
    spare,
    spare_got,
    admissible,
    gain,
    plan,
    load_sem,
    wo_sem,
    ctx_sem,
    part_sem,
    sum_sem,
    end_sem,
):
    sections = lax.axis_size("section")
    section = lax.axis_index("section")
    tp = lax.axis_index("tp")
    count = side * side
    z, y = tp // side, tp % side
    place = (z, y)
    final = sections - 1
    following = (section + 1) % sections
    before = (section + final) % sections
    rows, width = pending.shape[0], pending.shape[1]
    part = rows // CHUNKS
    cols = width // count
    halves = cols // LANES

    def send(src, dst, sems, where):
        copy = pltpu.make_async_remote_copy(
            src_ref=src,
            dst_ref=dst,
            send_sem=sems.at[0],
            recv_sem=sems.at[1],
            device_id=where,
            device_id_type=MESH,
        )
        copy.start()

    def on_line(line, step):
        if line == 0:
            return ((z + step) % side) * side + y
        return z * side + (y + step) % side

    far_first = [2, 1, 3] if side == 4 else list(range(1, side))

    barrier = pltpu.get_barrier_semaphore()
    senders = [(section, on_line(line, d)) for line in range(2) for d in range(1, side)]
    senders += [(before, on_line(0, d)) for d in range(side)]
    senders += [(before, on_line(1, d)) for d in range(1, side)]
    for sender in senders:
        pl.semaphore_signal(barrier, inc=1, device_id=sender, device_id_type=MESH)
    smalls = [
        pltpu.make_async_copy(src, dst, load_sem.at[6 + i])
        for i, (src, dst) in enumerate(
            ((plan_hbm, plan), (gain_hbm, gain), (admissible_hbm, admissible))
        )
    ]
    for load in smalls:
        load.start()
    load_x = pltpu.make_async_copy(pending, x_raw, load_sem.at[0])
    load_x.start()
    loads = [
        pltpu.make_async_copy(
            w_in_hbm.at[j], w_in.at[:, pl.ds(j * HD, HD)], load_sem.at[1 + j]
        )
        for j in range(3)
    ]
    for load in loads:
        load.start()

    def columns(line, peer_at, q):
        block = peer_at * side + q if line == 0 else q * side + peer_at
        return w_out_hbm.at[:, pl.ds(pl.multiple_of(block * cols + line * LANES, LANES), LANES)]

    for line in range(2):
        for q in range(side):
            pltpu.make_async_copy(
                columns(line, place[line], q),
                w_line.at[line, place[line], :, pl.ds(q * LANES, LANES)],
                load_sem.at[4 + line],
            ).start()
    pl.semaphore_wait(barrier, len(senders))
    for step in far_first:
        for line in range(2):
            for q in range(side):
                send(
                    columns(line, (place[line] + step) % side, q),
                    w_line.at[line, place[line], :, pl.ds(q * LANES, LANES)],
                    wo_sem.at[line],
                    (section, on_line(line, step)),
                )
    for load in smalls:
        load.wait()
    lost = vanished[0]
    late_wrap = (lost == final - 1) | (lost == final - 2)
    load_x.wait()
    for c in range(count):
        for h in range(halves):
            for r in range(CHUNKS):
                start = c * cols + h * LANES
                block = x_raw[r * part : (r + 1) * part, start : start + LANES]
                x[0, r, h, c // side, c % side] = jnp.where(
                    section == lost, jnp.zeros_like(block), block
                )
    for load in loads:
        load.wait()

    def heads(k, r):
        def blocks():
            for c in range(count):
                for h in range(halves):
                    yield c * cols + h * LANES, x[k, r, h, c // side, c % side].astype(jnp.float32)

        summed = jnp.zeros((part, LANES), jnp.float32)
        for _, block in blocks():
            summed = summed + block
        mean = jnp.sum(summed, axis=-1, keepdims=True) * (1.0 / width)
        summed = jnp.zeros((part, LANES), jnp.float32)
        for _, block in blocks():
            block = block - mean
            summed = summed + block * block
        scale = lax.rsqrt(jnp.sum(summed, axis=-1, keepdims=True) * (1.0 / width) + NORM_EPS)
        for at, block in blocks():
            g = gain[:, at : at + LANES].astype(jnp.float32)
            normed[:, at : at + LANES] = ((block - mean) * scale * g).astype(jnp.bfloat16)
        projected = jnp.dot(normed[...], w_in[...], preferred_element_type=jnp.float32).astype(
            jnp.bfloat16
        )
        keys[r * part : (r + 1) * part, :] = projected[:, HD : 2 * HD]
        values[r * part : (r + 1) * part, :] = projected[:, 2 * HD :]
        seen = (r + 1) * part
        scores = lax.dot_general(
            projected[:, :HD],
            keys[:seen, :],
            (((1,), (1,)), ((), ())),
            preferred_element_type=jnp.float32,
        ) * HD ** (-0.5)
        row = lax.broadcasted_iota(jnp.int32, (part, seen), 0) + r * part
        col = lax.broadcasted_iota(jnp.int32, (part, seen), 1)
        scores = jnp.where(row >= col, scores, -jnp.inf)
        weights = jnp.exp(scores - jnp.max(scores, axis=-1, keepdims=True))
        probs = (weights / jnp.sum(weights, axis=-1, keepdims=True)).astype(jnp.bfloat16)
        mixed = jnp.dot(probs, values[:seen, :], preferred_element_type=jnp.float32)
        mixed = mixed.astype(jnp.bfloat16)
        for line in range(2):
            ctx[k, r, line, place[line]] = mixed
        for step in far_first:
            for line in range(2):
                block = ctx.at[k, r, line, place[line]]
                send(block, block, ctx_sem.at[k, r, line], (section, on_line(line, step)))

    def mix(k, r):
        early = (following == (lost + 2) % sections) & (lost <= final - 1)
        late = ((following == (lost + 3) % sections) & (lost <= final - 1)) | (
            (following == (lost + 4) % sections) & (lost <= final - 2)
        )
        enters = (k < 2) | ((k == 2) & late_wrap) | ((k == 3) & jnp.logical_not(late_wrap))
        enters = enters & (section == final)
        holds = (k == 2) & (lost == final) & (section == final)
        for line in range(2):
            arrive(ctx.at[k, r, line, pl.ds(0, side - 1)], ctx_sem.at[k, r, line, 1])
            context = jnp.concatenate([ctx[k, r, line, i] for i in range(side)], axis=1)
            branch = jnp.dot(
                context,
                w_line[line].reshape(side * HD, side * LANES),
                preferred_element_type=jnp.float32,
            )
            across = place[1 - line]
            for q in range(side):
                block = x[k, r, 0, z, q] if line == 0 else x[k, r, 1, q, y]
                share = branch[:, q * LANES : (q + 1) * LANES] + jnp.where(
                    across == q, block.astype(jnp.float32), 0.0
                )
                kept[k, r, line, q] = share.astype(jnp.bfloat16)

            @pl.when(k < SLOTS - 1)
            def _():
                entering = admissible[
                    plan[jnp.minimum(k, 2)],
                    r * part : (r + 1) * part,
                    line * LANES : (line + 1) * LANES,
                ]
                for q in range(side):
                    fresh = jnp.where(across == q, entering, jnp.zeros_like(entering))
                    value = jnp.where(holds, kept[0, r, line, q], kept[k, r, line, q])
                    sent[k, r, line, q] = jnp.where(enters, fresh, value)
                if line == 0:
                    for step in [*far_first, 0]:
                        send(
                            sent.at[k, r, 0],
                            got.at[k, r, 0, y],
                            part_sem.at[k, r, 0],
                            (following, on_line(1, step)),
                        )
                else:
                    for step in far_first:
                        send(
                            sent.at[k, r, 1],
                            got.at[k, r, 1, z],
                            part_sem.at[k, r, 1],
                            (section, on_line(0, step)),
                        )
                    for q in range(side):
                        got[k, r, 1, z, q] = sent[k, r, 1, q]

            @pl.when(k == SLOTS - 1)
            def _():
                for q in range(side):
                    value = jnp.where(late, kept[k, r, line, q], kept[3, r, line, q])
                    spare[r, line, q] = jnp.where(early, kept[1, r, line, q], value)
                for q in range(side):
                    send(
                        spare.at[r, line, q],
                        spare_got.at[r, line, across],
                        end_sem.at[r, line],
                        (following, z * side + q if line == 0 else q * side + y),
                    )

    def summed(k, r, line, q):
        value = got[k, r, line, 0, q].astype(jnp.float32)
        for i in range(1, side):
            value = value + got[k, r, line, i, q].astype(jnp.float32)
        return value.astype(jnp.bfloat16)

    def forward(k, r):
        arrive(got.at[k, r, 1, pl.ds(0, side - 1)], part_sem.at[k, r, 1, 1])
        for q in range(side):
            total[k, r, q] = summed(k, r, 1, q)
        for step in [*far_first, 0]:
            send(
                total.at[k, r],
                x.at[k + 1, r, 1, :, y],
                sum_sem.at[k, r, 1],
                (following, on_line(1, step)),
            )
        arrive(got.at[k, r, 0], part_sem.at[k, r, 0, 1])
        for q in range(side):
            x[k + 1, r, 0, z, q] = summed(k, r, 0, q)
        for step in far_first:
            block = x.at[k + 1, r, 0, z]
            send(block, block, sum_sem.at[k, r, 0], (section, on_line(0, step)))

    def gathered(k, r):
        arrive(x.at[k + 1, r, 0, pl.ds(0, side - 1)], sum_sem.at[k, r, 0, 1])
        arrive(x.at[k + 1, r, 1], sum_sem.at[k, r, 1, 1])

    def left(k):
        for r in range(CHUNKS):
            for line in range(2):
                arrive(ctx.at[k, r, line, pl.ds(0, side - 1)], ctx_sem.at[k, r, line, 0])
            arrive(got.at[k, r, 0], part_sem.at[k, r, 0, 0])
            arrive(got.at[k, r, 1, pl.ds(0, side - 1)], part_sem.at[k, r, 1, 0])
            arrive(x.at[k, r, 0, pl.ds(0, side - 1)], sum_sem.at[k, r, 0, 0])
            arrive(x.at[k, r, 1], sum_sem.at[k, r, 1, 0])

    def slot(k, carry):
        for r in range(CHUNKS):

            @pl.when(k > 0)
            def _():
                gathered(k - 1, r)

            heads(k, r)

        @pl.when(k == 0)
        def _():
            for line in range(2):
                arrive(w_line.at[line, 0], load_sem.at[4 + line])
                arrive(w_line.at[line, pl.ds(0, side - 1)], wo_sem.at[line, 1])

        @pl.when(k == SLOTS - 1)
        def _():
            for line in range(2):
                arrive(w_line.at[line, pl.ds(0, side - 1)], wo_sem.at[line, 0])
            behind = (section > lost) & (section <= lost + 3)
            newest = jnp.where(section == 0, jnp.logical_not(late_wrap), behind)
            for c in range(count):
                for h in range(halves):
                    for r in range(CHUNKS):
                        at = (r, h, c // side, c % side)
                        block = jnp.where(newest, x[SLOTS - 1, *at], x[SLOTS - 2, *at])
                        block = jnp.where(section == lost, jnp.zeros_like(block), block)
                        start = c * cols + h * LANES
                        out_ref[r * part : (r + 1) * part, start : start + LANES] = block

        @pl.when(k > 0)
        def _():
            left(k - 1)

        for r in range(CHUNKS):
            mix(k, r)

        @pl.when(k < SLOTS - 1)
        def _():
            for r in range(CHUNKS):
                forward(k, r)

        return carry

    lax.fori_loop(0, SLOTS, slot, 0)

    for r in range(CHUNKS):
        for line in range(2):
            arrive(spare_got.at[r, line], end_sem.at[r, line, 1])
            value = spare_got[r, line, 0].astype(jnp.float32)
            for i in range(1, side):
                value = value + spare_got[r, line, i].astype(jnp.float32)
            standby_ref[r * part : (r + 1) * part, line * LANES : (line + 1) * LANES] = (
                value.astype(jnp.bfloat16)
            )
    for r in range(CHUNKS):
        for line in range(2):
            arrive(ctx.at[SLOTS - 1, r, line, pl.ds(0, side - 1)], ctx_sem.at[SLOTS - 1, r, line, 0])
            arrive(spare.at[r, line], end_sem.at[r, line, 0])


def in_hbm(array):
    return pltpu.with_memory_space_constraint(array, pltpu.HBM)


def per_device(pending, admissible, plan, vanished_hop, w_in, w_out, gain):
    count = lax.axis_size("tp")
    side = int(round(count**0.5))
    rows, width = pending.shape[1:]
    cols = width // count
    part = rows // CHUNKS
    halves = cols // LANES
    vmem = pl.BlockSpec(memory_space=pltpu.VMEM)
    smem = pl.BlockSpec(memory_space=pltpu.SMEM)
    hbm = pl.BlockSpec(memory_space=pltpu.HBM)
    bf16 = jnp.bfloat16
    dma = pltpu.SemaphoreType.DMA
    out, standby = pl.pallas_call(
        functools.partial(kernel, side),
        out_shape=(
            jax.ShapeDtypeStruct((rows, width), bf16),
            jax.ShapeDtypeStruct((rows, cols), bf16),
        ),
        in_specs=[hbm] * 3 + [smem] + [hbm] * 3,
        out_specs=(vmem, vmem),
        scratch_shapes=[
            pltpu.VMEM((rows, width), bf16),
            pltpu.VMEM((width, 3 * HD), bf16),
            pltpu.VMEM((2, side, HD, side * LANES), bf16),
            pltpu.VMEM((SLOTS, CHUNKS, halves, side, side, part, LANES), bf16),
            pltpu.VMEM((SLOTS, CHUNKS, 2, side, part, HD), bf16),
            pltpu.VMEM((SLOTS, CHUNKS, 2, side, part, LANES), bf16),
            pltpu.VMEM((SLOTS - 1, CHUNKS, 2, side, part, LANES), bf16),
            pltpu.VMEM((SLOTS - 1, CHUNKS, 2, side, side, part, LANES), bf16),
            pltpu.VMEM((SLOTS - 1, CHUNKS, side, part, LANES), bf16),
            pltpu.VMEM((part, width), bf16),
            pltpu.VMEM((rows, HD), bf16),
            pltpu.VMEM((rows, HD), bf16),
            pltpu.VMEM((CHUNKS, 2, side, part, LANES), bf16),
            pltpu.VMEM((CHUNKS, 2, side, part, LANES), bf16),
            pltpu.VMEM(admissible.shape, bf16),
            pltpu.VMEM(gain.shape, bf16),
            pltpu.SMEM(plan.shape, jnp.int32),
            dma((9,)),
            dma((2, 2)),
            dma((SLOTS, CHUNKS, 2, 2)),
            dma((SLOTS - 1, CHUNKS, 2, 2)),
            dma((SLOTS - 1, CHUNKS, 2, 2)),
            dma((CHUNKS, 2, 2)),
        ],
        compiler_params=pltpu.CompilerParams(
            has_side_effects=True, vmem_limit_bytes=48 * 1024 * 1024, collective_id=0
        ),
        name="relay",
    )(
        in_hbm(pending[0]),
        in_hbm(admissible),
        in_hbm(plan),
        vanished_hop,
        in_hbm(jnp.moveaxis(w_in[0], 1, 0)),
        in_hbm(w_out[0]),
        in_hbm(gain),
    )
    return out[None], standby[None]


def solution(mesh):
    placed = (
        P("section", None, None),
        P(None, None, "tp"),
        P(),
        P(),
        P("section", None, None, "tp"),
        P("section", "tp", None),
        P("section", None),
    )
    return jax.shard_map(
        per_device,
        mesh=mesh,
        in_specs=placed,
        out_specs=(P("section", None, None), P("section", None, "tp")),
        check_vma=False,
    )
```
